32 devices in a mesh: gx: 2 (over core), gy: 16 (over z, y, x).
Axes of the slice: x: 2, y: 2, z: 4, core: 2. Of those that a mesh axis runs over, the one named last changes fastest.
Arguments:
- density: float32 [32, 256, 256], P('gx', 'gy'), may hold values from 0.5 to 2
- momentum: float32 [3, 32, 256, 256], P(None, 'gx', 'gy'), may hold values from -3 to 3
- energy: float32 [32, 256, 256], P('gx', 'gy'), may hold values from 1 to 3
- parcel_mass: float32 [262144], P(('gx', 'gy')), may hold values from 0.2 to 2
- droplet_velocity: float32 [3, 262144], P(None, ('gx', 'gy')), may hold values from -4 to 4
- parcel_temp: float32 [262144], P(('gx', 'gy')), may hold values from 0.1 to 4
- parcel_cell: int32 [3, 262144], P(None, ('gx', 'gy')), may hold values from 0 to 255, as said below
- parcel_count: int32 [32], P(('gx', 'gy')), may hold values from 2048 to 8192, as said below
Outputs:
- updated_fluid_density: float32 [32, 256, 256], P('gx', 'gy')
- updated_fluid_impulse: float32 [3, 32, 256, 256], P(None, 'gx', 'gy')
- energy_out: float32 [32, 256, 256], P('gx', 'gy')
- moved_state: float32 [5, 327680], P(None, ('gx', 'gy'))
- moved_cell: int32 [3, 327680], P(None, ('gx', 'gy'))
- time_step: float32 [], replicated
The draws below stay inside these ranges and needn't reach their ends.
Inputs may be any that keep to these rules, and one draw needn't show every extreme that they name: `parcel_cell`: each row of device d lies in d's block of 16 x 16 x 256 cells or in the layer of cells just beyond one of its four side faces inside the grid, never beyond an edge. Among the live rows of one device at most 512 lie beyond any one face; on every device some face along each of the two axes has exactly 512. `parcel_count`: some devices are full.
All inputs are finite; a program needn't handle non-finite values.
Results may differ from the reference program's by a relative error of at most 0.0003.
Values sent between devices are 32-bit elements; how exact they have to be, the bound alone decides.
A program may use at most 192 MiB of HBM per device.

```python
import math
import jax
import jax.numpy as jnp
from jax import lax

CX = 16
CY = 16
NZ = 256
P_DEV = 8192
MOVE = 512
SLOTS = 10240
NX = 32
NY = 256
PARCELS = 262144
N_GX = 2
N_GY = 16
DEVICES = 32


def parcel_state_tables(key):
    base = jax.random.fold_in(key, 11)
    keys = jax.random.split(base, 8)
    device = jnp.arange(DEVICES, dtype=jnp.int32)
    col_x = device // N_GY
    col_y = device % N_GY
    partial_parcel_count = jax.random.randint(keys[0], (DEVICES,), P_DEV // 4, P_DEV // 2 + 1, dtype=jnp.int32)
    count = jnp.where(col_x == 0, P_DEV, partial_parcel_count).astype(jnp.int32)
    exists = jnp.stack([col_x > 0, col_x < N_GX - 1, col_y > 0, col_y < N_GY - 1], axis=1)
    loads = jax.random.randint(keys[1], (DEVICES, 4), MOVE // 4, MOVE + 1, dtype=jnp.int32)
    drag_horizontal = jnp.where(col_x < N_GX - 1, 1, 0)
    force_y = jnp.where(col_y < N_GY - 1, 3, 2)
    which = jnp.arange(4, dtype=jnp.int32)[None]
    loads = jnp.where((which == drag_horizontal[:, None]) | (which == force_y[:, None]), MOVE, loads)
    loads = jnp.where(exists, loads, 0)
    ends = jnp.cumsum(loads, axis=1)
    row_index = jnp.arange(P_DEV, dtype=jnp.int32)[None]
    spread = 2 ** 30 // (2 * P_DEV)
    scores = jax.random.randint(keys[2], (DEVICES, P_DEV), 0, spread, dtype=jnp.int32) * P_DEV + row_index
    scores = jnp.where(row_index < count[:, None], scores, 2 ** 30 + row_index)
    order = jnp.argsort(scores, axis=1, stable=True)
    position = jnp.argsort(order, axis=1, stable=True).astype(jnp.int32)
    heading = jnp.sum((position[:, :, None] >= ends[:, None, :]).astype(jnp.int32), axis=2)
    inside_x = jax.random.randint(keys[3], (DEVICES, P_DEV), 0, CX, dtype=jnp.int32) + col_x[:, None] * CX
    inside_y = jax.random.randint(keys[4], (DEVICES, P_DEV), 0, CY, dtype=jnp.int32) + col_y[:, None] * CY
    depth = jax.random.randint(keys[5], (DEVICES, P_DEV), 0, NZ, dtype=jnp.int32)
    cell_x = jnp.where(heading == 0, col_x[:, None] * CX - 1, jnp.where(heading == 1, col_x[:, None] * CX + CX, inside_x))
    cell_y = jnp.where(heading == 2, col_y[:, None] * CY - 1, jnp.where(heading == 3, col_y[:, None] * CY + CY, inside_y))
    cells = jnp.stack([cell_x, cell_y, depth]).reshape(3, DEVICES * P_DEV).astype(jnp.int32)
    return (cells, count)


def draw_parcel_cell(key, part):
    return parcel_state_tables(key)[0]


def draw_parcel_count(key, part):
    return parcel_state_tables(key)[1]


def level_of(stream_key, dims, cuts, smallest, top_value):
    loudness = 1.0
    for dim, blocks in cuts:
        heights = jax.random.uniform(jax.random.fold_in(jax.random.fold_in(stream_key, 6), dim), (blocks,), jnp.float32, smallest / len(cuts), top_value / len(cuts))
        loudness = loudness * jnp.repeat(jnp.exp(heights), dims[dim] // blocks).reshape((-1,) + (1,) * (len(dims) - 1 - dim))
    return loudness


def noise(stream_key, extent, deviation, reach, shards=(), held_as=jnp.bfloat16):
    values = jax.random.normal(stream_key, extent, jnp.float32) * deviation
    if len(shards) > 0:
        values = level_of(stream_key, extent, shards, -0.22, 0.18) * values
    return jnp.clip(values, min=-reach, max=reach).astype(held_as)


def setup_inputs(seed: int = 0) -> dict:
    key_of = jax.random.split(jax.random.key(seed), 9)
    density = jnp.clip(0.5 + 1.5 * jax.random.uniform(key_of[0], (NX, NY, NZ), jnp.float32) ** level_of(key_of[0], (NX, NY, NZ), ((0, 2), (1, 16)), -0.2, 0.2), 0.5, 2.0)
    momentum = noise(key_of[1], (3, NX, NY, NZ), 0.5, 3.0, ((1, 2), (2, 16)), jnp.float32)
    energy = jnp.clip(1.0 + 2.0 * jax.random.uniform(key_of[2], (NX, NY, NZ), jnp.float32) ** level_of(key_of[2], (NX, NY, NZ), ((0, 2), (1, 16)), -0.2, 0.2), 1.0, 3.0)
    parcel_mass = jnp.clip(jnp.exp(math.log(2.0) - 2.3025851 * jax.random.uniform(key_of[3], (PARCELS,), jnp.float32) ** level_of(key_of[3], (PARCELS,), ((0, 32),), -0.2, 0.2)), 0.2, 2.0)
    droplet_velocity = noise(key_of[4], (3, PARCELS), 1.0, 4.0, ((1, 32),), jnp.float32)
    parcel_temp = jnp.clip(0.1 + 3.9 * jax.random.uniform(key_of[5], (PARCELS,), jnp.float32) ** level_of(key_of[5], (PARCELS,), ((0, 32),), -0.2, 0.2), 0.1, 4.0)
    parcel_cell = draw_parcel_cell(jax.random.fold_in(key_of[8], 71), 0)
    parcel_count = draw_parcel_count(jax.random.fold_in(key_of[8], 71), 0)
    return dict(density=density, momentum=momentum, energy=energy, parcel_mass=parcel_mass, droplet_velocity=droplet_velocity, parcel_temp=parcel_temp, parcel_cell=parcel_cell, parcel_count=parcel_count)


ADIABATIC_INDEX = 1.4
KICK = 0.25
COURANT = 0.4
SHRINK = 0.5

def cell_sums(values, cell_ids, segments):
    return jax.ops.segment_sum(values, cell_ids, num_segments=segments)

def reference(density, momentum, energy, parcel_mass, droplet_velocity, parcel_temp, parcel_cell, parcel_count):
    row_index = jnp.arange(parcel_mass.shape[0], dtype=jnp.int32)
    device = row_index // P_DEV
    local_row = row_index % P_DEV
    live = local_row < parcel_count[device]
    boiled_off_amount = jnp.where(live, parcel_mass * jax.nn.sigmoid(2.0 * (parcel_temp - 2.0)), 0.0)
    specific_movement_budget = 0.5 * lax.optimization_barrier(jnp.sum(droplet_velocity * droplet_velocity, axis=0))
    sources = jnp.concatenate([boiled_off_amount[None], boiled_off_amount[None] * droplet_velocity, (boiled_off_amount * (parcel_temp + specific_movement_budget))[None]], axis=0)
    flat_cell = (parcel_cell[0] * NY + parcel_cell[1]) * NZ + parcel_cell[2]
    deposit = jax.vmap(lambda values: cell_sums(values, flat_cell, NX * NY * NZ))(sources).reshape(5, NX, NY, NZ)
    updated_fluid_density = density + deposit[0]
    energy_out = energy + deposit[4]
    lifted = momentum + deposit[1:4]
    normal_stress_field = (ADIABATIC_INDEX - 1.0) * energy_out
    padded = jnp.pad(normal_stress_field, 1)
    grad_x = 0.5 * (padded[2:, 1:-1, 1:-1] - padded[:-2, 1:-1, 1:-1])
    grad_y = 0.5 * (padded[1:-1, 2:, 1:-1] - padded[1:-1, :-2, 1:-1])
    grad_z = 0.5 * (padded[1:-1, 1:-1, 2:] - padded[1:-1, 1:-1, :-2])
    updated_fluid_impulse = lifted - KICK * jnp.stack([grad_x, grad_y, grad_z])
    ambient_stream_speed = updated_fluid_impulse / updated_fluid_density[None]
    acoustic_signal = lax.optimization_barrier(jnp.max(jnp.abs(ambient_stream_speed), axis=0)) + jnp.sqrt(ADIABATIC_INDEX * normal_stress_field / updated_fluid_density)
    time_step = COURANT / jnp.max(acoustic_signal)
    col_x = device // N_GY
    col_y = device % N_GY
    local_x = parcel_cell[0] - col_x * CX
    local_y = parcel_cell[1] - col_y * CY
    heading = jnp.where(local_x < 0, 0, jnp.where(local_x >= CX, 1, jnp.where(local_y < 0, 2, jnp.where(local_y >= CY, 3, 4))))
    heading = jnp.where(live, heading, 5).astype(jnp.int32)
    onehot = (heading[:, None] == jnp.arange(4, dtype=jnp.int32)[None]).astype(jnp.int32).reshape(DEVICES, P_DEV, 4)
    earlier = (jnp.cumsum(onehot, axis=1) - onehot).reshape(DEVICES * P_DEV, 4)
    rank = lax.optimization_barrier(jnp.sum(earlier * onehot.reshape(DEVICES * P_DEV, 4), axis=1))
    shift_table = jnp.array([-N_GY, N_GY, -1, 1, 0, 0], dtype=jnp.int32)
    bucket_table = jnp.array([1, 0, 3, 2, 0, 0], dtype=jnp.int32)
    target_dev = device + shift_table[heading]
    moving = jnp.where(heading < 4, target_dev * SLOTS + P_DEV + bucket_table[heading] * MOVE + rank, SLOTS * DEVICES)
    target = jnp.where(heading == 4, device * SLOTS + local_row, moving).astype(jnp.int32)
    carried_records = jnp.concatenate([(parcel_mass - SHRINK * boiled_off_amount)[None], droplet_velocity, parcel_temp[None], parcel_cell.astype(jnp.float32)], axis=0)
    table = jnp.zeros((8, SLOTS * DEVICES), carried_records.dtype).at[:, target].set(carried_records, mode='drop')
    moved_state = table[:5]
    moved_cell = table[5:].astype(jnp.int32)
    return (updated_fluid_density, updated_fluid_impulse, energy_out, moved_state, moved_cell, time_step)
```

```python
import functools

import jax
import jax.numpy as jnp
from jax import lax
from jax.experimental import pallas as pl
from jax.experimental.pallas import tpu as pltpu
from jax.sharding import PartitionSpec as P

ADIABATIC_INDEX = 1.4
KICK = 0.25
COURANT = 0.4
SHRINK = 0.5
MESH = pl.DeviceIdType.MESH
CHUNK = 1024
F32 = jnp.float32
BF16 = jnp.bfloat16
F8 = jnp.float8_e4m3fn
LIFT = 512.0
EDGES_AT = 2


def dot_nt(a, b):
    return lax.dot_general(a, b, (((1,), (1,)), ((), ())), preferred_element_type=F32)


def two_terms(x):
    high = x.astype(BF16)
    low = (x - high.astype(F32)).astype(BF16)
    return high, low


def one_hot_rows(row, count):
    lanes = row.shape[1]
    base = (
        jnp.broadcast_to(row, (16, lanes))
        - lax.broadcasted_iota(jnp.int32, (16, lanes), 0).astype(F32)
    ).astype(BF16)
    one, zero = jnp.ones((16, lanes), BF16), jnp.zeros((16, lanes), BF16)
    return jnp.concatenate(
        [jnp.where(base == 16.0 * k, one, zero) for k in range(count // 16)], axis=0
    )


def peers_of(n_gx, n_gy):
    both = [(a, b) for a in range(n_gx) for b in range(n_gy) if a or b]
    if n_gx * n_gy <= 64:
        return (both,)
    return ([p for p in both if p[1] == 0], [p for p in both if p[0] == 0])


def kernel(
    n_gx, n_gy, count_ref, density_hbm, momentum_hbm, energy_hbm, mass_hbm, vel_hbm, temp_hbm, cell_hbm,
    rho_ref, imp_ref, en_ref, state_ref, moved_ref, step_ref,
    src_ref, pay_ref, col_ref, q_ref, r_ref, a0_ref, a1_ref, c0_ref, c1_ref, b_ref, d_ref, small_ref, inv_ref, sound_ref,
    out_bucket, in_bucket, out_face, in_face,
    bucket_send, bucket_recv, face_send, face_recv, max_send, max_recv,
    mass_ref, vel_ref, temp_ref, cell_ref, load_sem, *slots_refs,
):
    sources = (mass_hbm, temp_hbm, vel_hbm, cell_hbm, energy_hbm, density_hbm, momentum_hbm)
    places = (mass_ref, temp_ref, vel_ref, cell_ref, en_ref, rho_ref, imp_ref)
    loads = []
    for k in range(7):
        load = pltpu.make_async_copy(sources[k], places[k], load_sem.at[k])
        load.start()
        loads.append(load)
    gx, gy = lax.axis_index("gx"), lax.axis_index("gy")
    cx, cy, nz = rho_ref.shape
    rows = mass_ref.shape[1]
    cap = rows // 16
    per = cap // 128
    cells = cx * cy
    chunks = rows // CHUNK
    in_bucket[...] = jnp.zeros_like(in_bucket)
    in_face[...] = jnp.zeros_like(in_face)

    def peer(a, b):
        return {"gx": lax.rem(gx + a, n_gx), "gy": lax.rem(gy + b, n_gy)}

    rounds = peers_of(n_gx, n_gy)
    greeted = [p for group in rounds for p in group]
    barrier = pltpu.get_barrier_semaphore()
    for p in greeted:
        pl.semaphore_signal(barrier, inc=1, device_id=peer(*p), device_id_type=MESH)

    for load in loads[:4]:
        load.wait()
    mass, temp = mass_ref[...], temp_ref[...]
    live = lax.broadcasted_iota(jnp.int32, (1, rows), 1) < count_ref[0]
    evap = jnp.where(live, mass * jax.nn.sigmoid(2.0 * (temp - 2.0)), 0.0)
    vx, vy, vz = vel_ref[0:1, :], vel_ref[1:2, :], vel_ref[2:3, :]
    src_ref[0:1, :] = evap
    src_ref[1:2, :] = evap * vx
    src_ref[2:3, :] = evap * vy
    src_ref[3:4, :] = evap * vz
    src_ref[4:5, :] = evap * (temp + 0.5 * (vx * vx + vy * vy + vz * vz))
    pay_ref[0:1, :] = mass - SHRINK * evap
    pay_ref[1:4, :] = vel_ref[...]
    pay_ref[4:5, :] = temp
    pay_ref[5:8, :] = cell_ref[...].astype(F32)
    lx = cell_ref[0:1, :] - gx * cx
    ly = cell_ref[1:2, :] - gy * cy
    heading = jnp.where(
        lx < 0, 0, jnp.where(lx >= cx, 1, jnp.where(ly < 0, 2, jnp.where(ly >= cy, 3, 4)))
    )
    heading = jnp.where(live, heading, 5)
    stays = heading == 4
    col_ref[...] = jnp.where(stays, lx * cy + ly, -1000).astype(F32)
    state_ref[:, :rows] = jnp.where(stays, pay_ref[0:5, :], 0.0)
    moved_ref[:, :rows] = jnp.where(stays, cell_ref[...], 0)

    blocks = rows // 128
    marks = jnp.where(
        jnp.broadcast_to(heading, (8, rows)) == lax.broadcasted_iota(jnp.int32, (8, rows), 0), 1.0, 0.0
    )
    stacked = jnp.concatenate([marks[:, k * 128 : (k + 1) * 128] for k in range(blocks)], axis=0)
    i0 = lax.broadcasted_iota(jnp.int32, (128, 256), 0)
    i1 = lax.broadcasted_iota(jnp.int32, (128, 256), 1)
    upper = jnp.where((i0 < i1) | (i1 >= 128), 1.0, 0.0).astype(BF16)
    sums = jnp.dot(stacked.astype(BF16), upper, preferred_element_type=F32)
    carry = jnp.zeros((8, 128), F32)
    ranks = []
    for k in range(blocks):
        part = sums[k * 8 : (k + 1) * 8]
        mark = stacked[k * 8 : (k + 1) * 8]
        ranks.append(jnp.sum((part[:, :128] + carry) * mark, axis=0, keepdims=True))
        carry = carry + part[:, 128:]
    rank = jnp.concatenate(ranks, axis=1).astype(jnp.int32)
    q_ref[...] = jnp.where(heading < 4, heading * per + (rank >> 7), -1).astype(F32)
    r_ref[...] = (rank & 127).astype(F32)

    groups = 4 * per
    small_ref[...] = jnp.zeros_like(small_ref)

    def columns(lanes):
        base = (
            jnp.broadcast_to(col_ref[:, lanes], (16, CHUNK))
            - lax.broadcasted_iota(jnp.int32, (16, CHUNK), 0).astype(F32)
        ).astype(BF16)
        return [base == 16.0 * k for k in range(cells // 16)]

    def spread(v, lanes, hits):
        zero = jnp.zeros((16, CHUNK), BF16)
        value = jnp.broadcast_to(src_ref[v : v + 1, lanes], (16, CHUNK))
        high = value.astype(BF16)
        low = ((value - high.astype(F32)) * LIFT).astype(BF16)
        first = [jnp.where(hits[k], high, zero) for k in range(cells // 16)]
        second = [
            jnp.concatenate([jnp.where(hits[k], low, zero), jnp.where(hits[k + 1], low, zero)], axis=0).astype(F8)
            for k in range(0, cells // 16, 2)
        ]
        return first, second

    def front(c):
        lanes = pl.ds(pl.multiple_of(c * CHUNK, CHUNK), CHUNK)
        high, low = two_terms(pay_ref[:, lanes])
        both = jnp.concatenate([high.astype(F32), low.astype(F32)], axis=0).astype(BF16)
        q = jnp.broadcast_to(q_ref[:, lanes], (16, CHUNK)).astype(BF16)
        zero = jnp.zeros((16, CHUNK), BF16)
        left = jnp.concatenate([jnp.where(q == float(k), both, zero) for k in range(groups)], axis=0)
        small_ref[...] += dot_nt(left, one_hot_rows(r_ref[:, lanes], 128))
        depth = one_hot_rows(cell_ref[2:3, lanes].astype(F32), nz)
        unit = (depth * (1.0 / LIFT)).astype(F8)
        b_ref[c] = depth
        d_ref[c] = unit
        first, second = spread(4, lanes, columns(lanes))
        part = dot_nt(jnp.concatenate(first, axis=0), depth) + dot_nt(jnp.concatenate(second, axis=0), unit)
        en_ref[...] += part.reshape(cx, cy, nz)

    def two_front(i, carry):
        front(2 * i)
        front(2 * i + 1)
        return carry

    loads[4].wait()
    lax.fori_loop(0, chunks // 2, two_front, 0)
    for h in range(4):
        for j in range(per):
            k = (h * per + j) * 16
            out_bucket[h, :, j * 128 : (j + 1) * 128] = small_ref[k : k + 8, :] + small_ref[k + 8 : k + 16, :]

    def build(c, a_ref, c_ref):
        lanes = pl.ds(pl.multiple_of(c * CHUNK, CHUNK), CHUNK)
        hits = columns(lanes)
        for v in range(4):
            first, second = spread(v, lanes, hits)
            for k in range(cells // 16):
                at = v * cells + k * 16
                a_ref[at : at + 16, :] = first[k]
            for k in range(cells // 32):
                at = v * cells + k * 32
                c_ref[at : at + 32, :] = second[k]

    build(0, a0_ref, c0_ref)

    pl.semaphore_wait(barrier, len(greeted))

    targets = (
        {"gx": lax.rem(gx + n_gx - 1, n_gx)},
        {"gx": lax.rem(gx + 1, n_gx)},
        {"gy": lax.rem(gy + n_gy - 1, n_gy)},
        {"gy": lax.rem(gy + 1, n_gy)},
    )
    there = (gx > 0, gx < n_gx - 1, gy > 0, gy < n_gy - 1)
    landing = (1, 0, 3, 2)

    def link(h, src, dst, send, recv):
        return pltpu.make_async_remote_copy(
            src_ref=src.at[h], dst_ref=dst.at[landing[h]], send_sem=send.at[h],
            recv_sem=recv.at[landing[h]], device_id=targets[h], device_id_type=MESH,
        )

    def launch(*refs):
        for h in range(4):
            pl.when(there[h])(lambda h=h: link(h, *refs).start())

    def arrive(*refs):
        for h in range(4):
            pl.when(there[landing[h]])(lambda h=h: link(h, *refs).wait_recv())

    def depart(*refs):
        for h in range(4):
            pl.when(there[h])(lambda h=h: link(h, *refs).wait_send())

    moves = (out_bucket, in_bucket, bucket_send, bucket_recv)
    faces = (out_face, in_face, face_send, face_recv)
    launch(*moves)
    for load in loads[5:]:
        load.wait()

    def edges():
        arrive(*moves)
        for b in range(4):
            got = in_bucket[b]
            state_ref[:, rows + b * cap : rows + (b + 1) * cap] = got[0:5]
            moved_ref[:, rows + b * cap : rows + (b + 1) * cap] = got[5:8].astype(jnp.int32)
            warm = got[4:5]
            share = jax.nn.sigmoid(2.0 * (warm - 2.0))
            boiled = got[0:1] * share / (1.0 - SHRINK * share)
            speed = got[1:4]
            budget = 0.5 * jnp.sum(speed * speed, axis=0, keepdims=True)
            values = [boiled] + [boiled * got[k : k + 1] for k in (1, 2, 3)] + [boiled * (warm + budget)]
            if b < 2:
                along = got[6:7] - (gy * cy).astype(F32)
            else:
                along = got[5:6] - (gx * cx).astype(F32)
            hit = (
                jnp.broadcast_to(along, (16, cap))
                == lax.broadcasted_iota(jnp.int32, (16, cap), 0).astype(F32)
            )
            parts = []
            for value in values:
                wide = jnp.where(hit, jnp.broadcast_to(value, (16, cap)), 0.0)
                parts.append(two_terms(wide))
            left = jnp.concatenate([p[0] for p in parts] + [p[1] for p in parts], axis=0)
            sums = dot_nt(left, one_hot_rows(got[7:8], nz))
            sums = sums[0 : 5 * 16] + sums[5 * 16 : 10 * 16]
            fields = (rho_ref, imp_ref.at[0], imp_ref.at[1], imp_ref.at[2], en_ref)
            for v in range(5):
                part = sums[v * 16 : (v + 1) * 16]
                if b < 2:
                    x = 0 if b == 0 else cx - 1
                    fields[v][x] += part
                else:
                    y = 0 if b == 2 else cy - 1
                    for x in range(cx):
                        fields[v][x, y : y + 1, :] += part[x : x + 1]
        scale = ADIABATIC_INDEX - 1.0
        out_face[0] = scale * en_ref[0]
        out_face[1] = scale * en_ref[cx - 1]
        for x in range(cx):
            out_face[2, x : x + 1, :] = scale * en_ref[x, 0:1, :]
            out_face[3, x : x + 1, :] = scale * en_ref[x, cy - 1 : cy, :]
        launch(*faces)

    def add(c, a_ref, c_ref):
        part = dot_nt(a_ref[...], b_ref[c]) + dot_nt(c_ref[...], d_ref[c])
        rho_ref[...] += part[:cells].reshape(cx, cy, nz)
        imp_ref[...] += part[cells:].reshape(3, cx, cy, nz)

    def two_chunks(i, carry):
        pl.when(i == EDGES_AT)(edges)
        add(2 * i, a0_ref, c0_ref)
        build(2 * i + 1, a1_ref, c1_ref)
        add(2 * i + 1, a1_ref, c1_ref)
        build(jnp.minimum(2 * i + 2, chunks - 1), a0_ref, c0_ref)
        return carry

    lax.fori_loop(0, chunks // 2, two_chunks, 0)

    pressure = (ADIABATIC_INDEX - 1.0) * en_ref[...]
    inverse = 1.0 / rho_ref[...]
    inv_ref[...] = inverse
    sound_ref[...] = jnp.sqrt(ADIABATIC_INDEX * pressure * inverse)
    lane = lax.broadcasted_iota(jnp.int32, (cx, cy, nz), 2)
    after = jnp.where(lane == nz - 1, 0.0, pltpu.roll(pressure, nz - 1, 2))
    before = jnp.where(lane == 0, 0.0, pltpu.roll(pressure, 1, 2))
    half = 0.5 * KICK
    imp_ref[2] -= half * (after - before)
    line = lax.broadcasted_iota(jnp.int32, (cx, cy, nz), 1)
    after = jnp.where(line == cy - 1, 0.0, pltpu.roll(pressure, cy - 1, 1))
    before = jnp.where(line == 0, 0.0, pltpu.roll(pressure, 1, 1))
    imp_ref[1] -= half * (after - before)
    none = jnp.zeros((1, cy, nz), F32)
    after = jnp.concatenate([pressure[1:], none], axis=0)
    before = jnp.concatenate([none, pressure[:-1]], axis=0)
    imp_ref[0] -= half * (after - before)
    arrive(*faces)
    imp_ref[0, 0] += half * in_face[0]
    imp_ref[0, cx - 1] -= half * in_face[1]
    for x in range(cx):
        imp_ref[1, x, 0:1, :] += half * in_face[2, x : x + 1, :]
        imp_ref[1, x, cy - 1 : cy, :] -= half * in_face[3, x : x + 1, :]
    fastest = jnp.maximum(jnp.maximum(jnp.abs(imp_ref[0]), jnp.abs(imp_ref[1])), jnp.abs(imp_ref[2]))
    wave = fastest * inv_ref[...] + sound_ref[...]
    wave = jnp.max(wave.reshape(cells, nz), axis=0, keepdims=True)
    top = functools.reduce(jnp.maximum, [wave[:, k * 128 : (k + 1) * 128] for k in range(nz // 128)])

    def everyone(slots, sem):
        rest = slots.at[pl.ds(1, slots.shape[0] - 1)]
        return pltpu.make_async_copy(rest, rest, sem)

    for t, group in enumerate(rounds):
        slots = slots_refs[t]
        slots[0] = top
        for k, p in enumerate(group):
            pltpu.make_async_remote_copy(
                src_ref=slots.at[0], dst_ref=slots.at[k + 1], send_sem=max_send.at[t],
                recv_sem=max_recv.at[t], device_id=peer(*p), device_id_type=MESH,
            ).start()
        everyone(slots, max_recv.at[t]).wait()
        top = jnp.max(slots[...], axis=0)
    step_ref[...] = COURANT / jnp.broadcast_to(jnp.max(top, axis=1, keepdims=True), (1, 128))
    depart(*moves)
    depart(*faces)
    for t in range(len(rounds)):
        everyone(slots_refs[t], max_send.at[t]).wait()


def put_out(*refs):
    count = (len(refs) - 1) // 2
    copies = []
    for k in range(count):
        copy = pltpu.make_async_copy(refs[k], refs[count + k], refs[-1].at[k])
        copy.start()
        copies.append(copy)
    for copy in copies:
        copy.wait()


def on_device(n_gx, n_gy, density, momentum, energy, mass, velocity, temp, cell, count):
    rows = mass.shape[0]
    cap = rows // 16
    slots = rows + 4 * cap
    cx, cy, nz = density.shape
    vmem = pl.BlockSpec(memory_space=pltpu.VMEM)
    cells = cx * cy
    rounds = peers_of(n_gx, n_gy)
    outs = pl.pallas_call(
        functools.partial(kernel, n_gx, n_gy),
        out_shape=(
            pltpu.VMEM(density.shape, F32),
            pltpu.VMEM(momentum.shape, F32),
            pltpu.VMEM(energy.shape, F32),
            pltpu.VMEM((5, slots), F32),
            pltpu.VMEM((3, slots), jnp.int32),
            pltpu.VMEM((1, 128), F32),
        ),
        in_specs=[pl.BlockSpec(memory_space=pltpu.SMEM)] + [pl.BlockSpec(memory_space=pltpu.HBM)] * 7,
        out_specs=(vmem,) * 6,
        scratch_shapes=[
            pltpu.VMEM((8, rows), F32),
            pltpu.VMEM((8, rows), F32),
            pltpu.VMEM((1, rows), F32),
            pltpu.VMEM((1, rows), F32),
            pltpu.VMEM((1, rows), F32),
            pltpu.VMEM((4 * cells, CHUNK), BF16),
            pltpu.VMEM((4 * cells, CHUNK), BF16),
            pltpu.VMEM((4 * cells, CHUNK), F8),
            pltpu.VMEM((4 * cells, CHUNK), F8),
            pltpu.VMEM((rows // CHUNK, nz, CHUNK), BF16),
            pltpu.VMEM((rows // CHUNK, nz, CHUNK), F8),
            pltpu.VMEM((4 * (cap // 128) * 16, 128), F32),
            pltpu.VMEM(density.shape, F32),
            pltpu.VMEM(density.shape, F32),
            pltpu.VMEM((4, 8, cap), F32),
            pltpu.VMEM((4, 8, cap), F32),
            pltpu.VMEM((4, cx, nz), F32),
            pltpu.VMEM((4, cx, nz), F32),
            pltpu.SemaphoreType.DMA((4,)),
            pltpu.SemaphoreType.DMA((4,)),
            pltpu.SemaphoreType.DMA((4,)),
            pltpu.SemaphoreType.DMA((4,)),
            pltpu.SemaphoreType.DMA((len(rounds),)),
            pltpu.SemaphoreType.DMA((len(rounds),)),
            pltpu.VMEM((1, rows), F32),
            pltpu.VMEM(velocity.shape, F32),
            pltpu.VMEM((1, rows), F32),
            pltpu.VMEM(cell.shape, jnp.int32),
            pltpu.SemaphoreType.DMA((7,)),
        ] + [pltpu.VMEM((len(group) + 1, 1, 128), F32) for group in rounds],
        compiler_params=pltpu.CompilerParams(
            collective_id=0, has_side_effects=True, vmem_limit_bytes=64200000
        ),
        name="spray",
    )(count, density, momentum, energy, mass.reshape(1, rows), velocity, temp.reshape(1, rows), cell)
    final = pl.pallas_call(
        put_out,
        out_shape=tuple(pltpu.HBM(o.shape, o.dtype) for o in outs[:5]),
        in_specs=[vmem] * 5,
        out_specs=(pl.BlockSpec(memory_space=pltpu.HBM),) * 5,
        scratch_shapes=[pltpu.SemaphoreType.DMA((5,))],
        compiler_params=pltpu.CompilerParams(vmem_limit_bytes=8 * 1024 * 1024),
        name="put_out",
    )(*outs[:5])
    return tuple(final) + (outs[5][0, 0],)


def solution(mesh):
    in_specs = (
        P("gx", "gy", None),
        P(None, "gx", "gy", None),
        P("gx", "gy", None),
        P(("gx", "gy")),
        P(None, ("gx", "gy")),
        P(("gx", "gy")),
        P(None, ("gx", "gy")),
        P(("gx", "gy")),
    )
    out_specs = (
        P("gx", "gy", None),
        P(None, "gx", "gy", None),
        P("gx", "gy", None),
        P(None, ("gx", "gy")),
        P(None, ("gx", "gy")),
        P(),
    )
    return jax.shard_map(
        functools.partial(on_device, mesh.shape["gx"], mesh.shape["gy"]),
        mesh=mesh, in_specs=in_specs, out_specs=out_specs, check_vma=False,
    )
```

```python
import functools

import jax
import jax.numpy as jnp
from jax import lax
from jax.experimental import pallas as pl
from jax.experimental.pallas import tpu as pltpu
from jax.sharding import PartitionSpec as P

ADIABATIC_INDEX = 1.4
KICK = 0.25
COURANT = 0.4
SHRINK = 0.5
MESH = pl.DeviceIdType.MESH
CHUNK = 1024
F32 = jnp.float32
BF16 = jnp.bfloat16
F8 = jnp.float8_e4m3fn
LIFT = 512.0
EDGES_AT = 2


def dot_nt(a, b):
    return lax.dot_general(a, b, (((1,), (1,)), ((), ())), preferred_element_type=F32)


def two_terms(x):
    high = x.astype(BF16)
    low = (x - high.astype(F32)).astype(BF16)
    return high, low


def one_hot_rows(row, count):
    lanes = row.shape[1]
    base = (
        jnp.broadcast_to(row, (16, lanes))
        - lax.broadcasted_iota(jnp.int32, (16, lanes), 0).astype(F32)
    ).astype(BF16)
    one, zero = jnp.ones((16, lanes), BF16), jnp.zeros((16, lanes), BF16)
    return jnp.concatenate(
        [jnp.where(base == 16.0 * k, one, zero) for k in range(count // 16)], axis=0
    )


def peers_of(n_gx, n_gy):
    both = [(a, b) for a in range(n_gx) for b in range(n_gy) if a or b]
    if n_gx * n_gy <= 64:
        return (both,)
    return ([p for p in both if p[1] == 0], [p for p in both if p[0] == 0])


def kernel(
    n_gx, n_gy, count_hbm, density_hbm, momentum_hbm, energy_hbm, mass_hbm, vel_hbm, temp_hbm, cell_hbm,
    rho_ref, imp_ref, en_ref, state_ref, moved_ref, step_ref,
    upper_ref, src_ref, pay_ref, col_ref, q_ref, r_ref, a0_ref, a1_ref, c0_ref, c1_ref, b_ref, d_ref, small_ref, inv_ref, sound_ref,
    out_bucket, in_bucket, out_face, in_face,
    bucket_send, bucket_recv, face_send, face_recv, max_send, max_recv,
    count_ref, mass_ref, vel_ref, temp_ref, cell_ref, load_sem, *slots_refs,
):
    sources = (count_hbm, mass_hbm, temp_hbm, vel_hbm, cell_hbm, energy_hbm, density_hbm, momentum_hbm)
    places = (count_ref, mass_ref, temp_ref, vel_ref, cell_ref, en_ref, rho_ref, imp_ref)
    loads = []
    for k in range(8):
        load = pltpu.make_async_copy(sources[k], places[k], load_sem.at[k])
        load.start()
        loads.append(load)
    gx, gy = lax.axis_index("gx"), lax.axis_index("gy")
    cx, cy, nz = rho_ref.shape
    rows = mass_ref.shape[1]
    cap = rows // 16
    per = cap // 128
    cells = cx * cy
    chunks = rows // CHUNK
    in_bucket[...] = jnp.zeros_like(in_bucket)
    in_face[...] = jnp.zeros_like(in_face)

    def peer(a, b):
        return {"gx": lax.rem(gx + a, n_gx), "gy": lax.rem(gy + b, n_gy)}

    rounds = peers_of(n_gx, n_gy)
    greeted = [p for group in rounds for p in group]
    barrier = pltpu.get_barrier_semaphore()
    for p in greeted:
        pl.semaphore_signal(barrier, inc=1, device_id=peer(*p), device_id_type=MESH)

    for load in loads[:5]:
        load.wait()
    blocks = CHUNK // 128
    i0 = lax.broadcasted_iota(jnp.int32, (128, 256), 0)
    i1 = lax.broadcasted_iota(jnp.int32, (128, 256), 1)
    upper_ref[...] = jnp.where((i0 < i1) | (i1 >= 128), 1.0, 0.0).astype(BF16)

    def prepare(c, carry):
        lanes = pl.ds(c * CHUNK, CHUNK)
        mass, temp = mass_ref[:, lanes], temp_ref[:, lanes]
        live = lax.broadcasted_iota(jnp.int32, (1, CHUNK), 1) + c * CHUNK < count_ref[0]
        evap = jnp.where(live, mass * jax.nn.sigmoid(2.0 * (temp - 2.0)), 0.0)
        vx, vy, vz = vel_ref[0:1, lanes], vel_ref[1:2, lanes], vel_ref[2:3, lanes]
        src_ref[0:1, lanes] = evap
        src_ref[1:2, lanes] = evap * vx
        src_ref[2:3, lanes] = evap * vy
        src_ref[3:4, lanes] = evap * vz
        src_ref[4:5, lanes] = evap * (temp + 0.5 * (vx * vx + vy * vy + vz * vz))
        pay_ref[0:1, lanes] = mass - SHRINK * evap
        pay_ref[1:4, lanes] = vel_ref[:, lanes]
        pay_ref[4:5, lanes] = temp
        pay_ref[5:8, lanes] = cell_ref[:, lanes].astype(F32)
        lx = cell_ref[0:1, lanes] - gx * cx
        ly = cell_ref[1:2, lanes] - gy * cy
        heading = jnp.where(
            lx < 0, 0, jnp.where(lx >= cx, 1, jnp.where(ly < 0, 2, jnp.where(ly >= cy, 3, 4)))
        )
        heading = jnp.where(live, heading, 5)
        col_ref[:, lanes] = jnp.where(heading == 4, lx * cy + ly, -1000).astype(F32)
        marks = jnp.where(
            jnp.broadcast_to(heading, (8, CHUNK)) == lax.broadcasted_iota(jnp.int32, (8, CHUNK), 0), 1.0, 0.0
        )
        stacked = jnp.concatenate([marks[:, k * 128 : (k + 1) * 128] for k in range(blocks)], axis=0)
        sums = jnp.dot(stacked.astype(BF16), upper_ref[...], preferred_element_type=F32)
        ranks = []
        for k in range(blocks):
            part = sums[k * 8 : (k + 1) * 8]
            mark = stacked[k * 8 : (k + 1) * 8]
            ranks.append(jnp.sum((part[:, :128] + carry) * mark, axis=0, keepdims=True))
            carry = carry + part[:, 128:]
        rank = jnp.concatenate(ranks, axis=1).astype(jnp.int32)
        q_ref[:, lanes] = jnp.where(heading < 4, heading * per + (rank >> 7), -1).astype(F32)
        r_ref[:, lanes] = (rank & 127).astype(F32)
        return carry

    groups = 4 * per
    small_ref[...] = jnp.zeros_like(small_ref)

    def columns(lanes):
        base = (
            jnp.broadcast_to(col_ref[:, lanes], (16, CHUNK))
            - lax.broadcasted_iota(jnp.int32, (16, CHUNK), 0).astype(F32)
        ).astype(BF16)
        return [base == 16.0 * k for k in range(cells // 16)]

    def spread(v, lanes, hits):
        zero = jnp.zeros((16, CHUNK), BF16)
        value = jnp.broadcast_to(src_ref[v : v + 1, lanes], (16, CHUNK))
        high = value.astype(BF16)
        low = ((value - high.astype(F32)) * LIFT).astype(BF16)
        first = [jnp.where(hits[k], high, zero) for k in range(cells // 16)]
        second = [
            jnp.concatenate([jnp.where(hits[k], low, zero), jnp.where(hits[k + 1], low, zero)], axis=0).astype(F8)
            for k in range(0, cells // 16, 2)
        ]
        return first, second

    def front(c):
        lanes = pl.ds(c * CHUNK, CHUNK)
        high, low = two_terms(pay_ref[:, lanes])
        both = jnp.concatenate([high.astype(F32), low.astype(F32)], axis=0).astype(BF16)
        q = jnp.broadcast_to(q_ref[:, lanes], (16, CHUNK)).astype(BF16)
        zero = jnp.zeros((16, CHUNK), BF16)
        left = jnp.concatenate([jnp.where(q == float(k), both, zero) for k in range(groups)], axis=0)
        small_ref[...] += dot_nt(left, one_hot_rows(r_ref[:, lanes], 128))
        depth = one_hot_rows(cell_ref[2:3, lanes].astype(F32), nz)
        unit = (depth * (1.0 / LIFT)).astype(F8)
        b_ref[c] = depth
        d_ref[c] = unit
        first, second = spread(4, lanes, columns(lanes))
        part = dot_nt(jnp.concatenate(first, axis=0), depth) + dot_nt(jnp.concatenate(second, axis=0), unit)
        en_ref[...] += part.reshape(cx, cy, nz)

    count = jnp.zeros((8, 128), F32)
    count = prepare(0, count)
    count = prepare(1, count)
    loads[5].wait()
    for c in range(chunks):
        if c + 2 < chunks:
            count = prepare(c + 2, count)
        front(c)
    for h in range(4):
        for j in range(per):
            k = (h * per + j) * 16
            out_bucket[h, :, j * 128 : (j + 1) * 128] = small_ref[k : k + 8, :] + small_ref[k + 8 : k + 16, :]

    def build(c, a_ref, c_ref):
        lanes = pl.ds(c * CHUNK if isinstance(c, int) else pl.multiple_of(c * CHUNK, CHUNK), CHUNK)
        hits = columns(lanes)
        for v in range(4):
            first, second = spread(v, lanes, hits)
            for k in range(cells // 16):
                at = v * cells + k * 16
                a_ref[at : at + 16, :] = first[k]
            for k in range(cells // 32):
                at = v * cells + k * 32
                c_ref[at : at + 32, :] = second[k]

    build(0, a0_ref, c0_ref)

    pl.semaphore_wait(barrier, len(greeted))

    targets = (
        {"gx": lax.rem(gx + n_gx - 1, n_gx)},
        {"gx": lax.rem(gx + 1, n_gx)},
        {"gy": lax.rem(gy + n_gy - 1, n_gy)},
        {"gy": lax.rem(gy + 1, n_gy)},
    )
    there = (gx > 0, gx < n_gx - 1, gy > 0, gy < n_gy - 1)
    landing = (1, 0, 3, 2)

    def link(h, src, dst, send, recv):
        return pltpu.make_async_remote_copy(
            src_ref=src.at[h], dst_ref=dst.at[landing[h]], send_sem=send.at[h],
            recv_sem=recv.at[landing[h]], device_id=targets[h], device_id_type=MESH,
        )

    def launch(*refs):
        for h in range(4):
            pl.when(there[h])(lambda h=h: link(h, *refs).start())

    def arrive(*refs):
        for h in range(4):
            pl.when(there[landing[h]])(lambda h=h: link(h, *refs).wait_recv())

    def depart(*refs):
        for h in range(4):
            pl.when(there[h])(lambda h=h: link(h, *refs).wait_send())

    moves = (out_bucket, in_bucket, bucket_send, bucket_recv)
    faces = (out_face, in_face, face_send, face_recv)
    launch(*moves)
    for load in loads[6:]:
        load.wait()

    def edges():
        arrive(*moves)
        for b in range(4):
            got = in_bucket[b]
            warm = got[4:5]
            share = jax.nn.sigmoid(2.0 * (warm - 2.0))
            boiled = got[0:1] * share / (1.0 - SHRINK * share)
            speed = got[1:4]
            budget = 0.5 * jnp.sum(speed * speed, axis=0, keepdims=True)
            values = [boiled] + [boiled * got[k : k + 1] for k in (1, 2, 3)] + [boiled * (warm + budget)]
            if b < 2:
                along = got[6:7] - (gy * cy).astype(F32)
            else:
                along = got[5:6] - (gx * cx).astype(F32)
            hit = (
                jnp.broadcast_to(along, (16, cap))
                == lax.broadcasted_iota(jnp.int32, (16, cap), 0).astype(F32)
            )
            parts = []
            for value in values:
                wide = jnp.where(hit, jnp.broadcast_to(value, (16, cap)), 0.0)
                parts.append(two_terms(wide))
            left = jnp.concatenate([p[0] for p in parts] + [p[1] for p in parts], axis=0)
            sums = dot_nt(left, one_hot_rows(got[7:8], nz))
            sums = sums[0 : 5 * 16] + sums[5 * 16 : 10 * 16]
            fields = (rho_ref, imp_ref.at[0], imp_ref.at[1], imp_ref.at[2], en_ref)
            for v in range(5):
                part = sums[v * 16 : (v + 1) * 16]
                if b < 2:
                    x = 0 if b == 0 else cx - 1
                    fields[v][x] += part
                else:
                    y = 0 if b == 2 else cy - 1
                    for x in range(cx):
                        fields[v][x, y : y + 1, :] += part[x : x + 1]
        scale = ADIABATIC_INDEX - 1.0
        out_face[0] = scale * en_ref[0]
        out_face[1] = scale * en_ref[cx - 1]
        for x in range(cx):
            out_face[2, x : x + 1, :] = scale * en_ref[x, 0:1, :]
            out_face[3, x : x + 1, :] = scale * en_ref[x, cy - 1 : cy, :]
        launch(*faces)

    def add(c, a_ref, c_ref):
        part = dot_nt(a_ref[...], b_ref[c]) + dot_nt(c_ref[...], d_ref[c])
        rho_ref[...] += part[:cells].reshape(cx, cy, nz)
        imp_ref[...] += part[cells:].reshape(3, cx, cy, nz)

    half = 0.5 * KICK

    def kick():
        pressure = (ADIABATIC_INDEX - 1.0) * en_ref[...]
        lane = lax.broadcasted_iota(jnp.int32, (cx, cy, nz), 2)
        after = jnp.where(lane == nz - 1, 0.0, pltpu.roll(pressure, nz - 1, 2))
        before = jnp.where(lane == 0, 0.0, pltpu.roll(pressure, 1, 2))

        imp_ref[2] -= half * (after - before)
        line = lax.broadcasted_iota(jnp.int32, (cx, cy, nz), 1)
        after = jnp.where(line == cy - 1, 0.0, pltpu.roll(pressure, cy - 1, 1))
        before = jnp.where(line == 0, 0.0, pltpu.roll(pressure, 1, 1))
        imp_ref[1] -= half * (after - before)
        none = jnp.zeros((1, cy, nz), F32)
        after = jnp.concatenate([pressure[1:], none], axis=0)
        before = jnp.concatenate([none, pressure[:-1]], axis=0)
        imp_ref[0] -= half * (after - before)

    def two_chunks(i, carry):
        add(2 * i, a0_ref, c0_ref)
        build(2 * i + 1, a1_ref, c1_ref)
        add(2 * i + 1, a1_ref, c1_ref)
        build(2 * i + 2, a0_ref, c0_ref)
        return carry

    head = EDGES_AT
    lax.fori_loop(0, head, two_chunks, 0)
    edges()
    for c in range(2 * head, chunks):
        a_ref, c_ref = ((a0_ref, c0_ref), (a1_ref, c1_ref))[c % 2]
        add(c, a_ref, c_ref)
        if c + 1 < chunks:
            build(c + 1, *((a1_ref, c1_ref), (a0_ref, c0_ref))[c % 2])
        if c == 2 * head:
            kick()

    inverse = 1.0 / rho_ref[...]
    inv_ref[...] = inverse
    sound_ref[...] = jnp.sqrt(ADIABATIC_INDEX * (ADIABATIC_INDEX - 1.0) * en_ref[...] * inverse)
    arrive(*faces)
    imp_ref[0, 0] += half * in_face[0]
    imp_ref[0, cx - 1] -= half * in_face[1]
    for x in range(cx):
        imp_ref[1, x, 0:1, :] += half * in_face[2, x : x + 1, :]
        imp_ref[1, x, cy - 1 : cy, :] -= half * in_face[3, x : x + 1, :]
    fastest = jnp.maximum(jnp.maximum(jnp.abs(imp_ref[0]), jnp.abs(imp_ref[1])), jnp.abs(imp_ref[2]))
    wave = fastest * inv_ref[...] + sound_ref[...]
    wave = jnp.max(wave.reshape(cells, nz), axis=0, keepdims=True)
    top = functools.reduce(jnp.maximum, [wave[:, k * 128 : (k + 1) * 128] for k in range(nz // 128)])

    def settle():
        stays = col_ref[...] >= 0.0
        state_ref[:, :rows] = jnp.where(stays, pay_ref[0:5, :], 0.0)
        moved_ref[:, :rows] = jnp.where(stays, cell_ref[...], 0)
        for b in range(4):
            got = in_bucket[b]
            state_ref[:, rows + b * cap : rows + (b + 1) * cap] = got[0:5]
            moved_ref[:, rows + b * cap : rows + (b + 1) * cap] = got[5:8].astype(jnp.int32)

    def everyone(slots, sem):
        rest = slots.at[pl.ds(1, slots.shape[0] - 1)]
        return pltpu.make_async_copy(rest, rest, sem)

    for t, group in enumerate(rounds):
        slots = slots_refs[t]
        slots[0] = top
        for k, p in enumerate(group):
            pltpu.make_async_remote_copy(
                src_ref=slots.at[0], dst_ref=slots.at[k + 1], send_sem=max_send.at[t],
                recv_sem=max_recv.at[t], device_id=peer(*p), device_id_type=MESH,
            ).start()
        if t == 0:
            settle()
        everyone(slots, max_recv.at[t]).wait()
        top = jnp.max(slots[...], axis=0)
    step_ref[...] = COURANT / jnp.broadcast_to(jnp.max(top, axis=1, keepdims=True), (1, 128))
    depart(*moves)
    depart(*faces)
    for t in range(len(rounds)):
        everyone(slots_refs[t], max_send.at[t]).wait()


def put_out(*refs):
    count = (len(refs) - 1) // 2
    copies = []
    for k in range(count):
        copy = pltpu.make_async_copy(refs[k], refs[count + k], refs[-1].at[k])
        copy.start()
        copies.append(copy)
    for copy in copies:
        copy.wait()


def on_device(n_gx, n_gy, density, momentum, energy, mass, velocity, temp, cell, count):
    rows = mass.shape[0]
    cap = rows // 16
    slots = rows + 4 * cap
    cx, cy, nz = density.shape
    vmem = pl.BlockSpec(memory_space=pltpu.VMEM)
    cells = cx * cy
    rounds = peers_of(n_gx, n_gy)
    outs = pl.pallas_call(
        functools.partial(kernel, n_gx, n_gy),
        out_shape=(
            pltpu.VMEM(density.shape, F32),
            pltpu.VMEM(momentum.shape, F32),
            pltpu.VMEM(energy.shape, F32),
            pltpu.VMEM((5, slots), F32),
            pltpu.VMEM((3, slots), jnp.int32),
            pltpu.VMEM((1, 128), F32),
        ),
        in_specs=[pl.BlockSpec(memory_space=pltpu.HBM)] * 8,
        out_specs=(vmem,) * 6,
        scratch_shapes=[
            pltpu.VMEM((128, 256), BF16),
            pltpu.VMEM((8, rows), F32),
            pltpu.VMEM((8, rows), F32),
            pltpu.VMEM((1, rows), F32),
            pltpu.VMEM((1, rows), F32),
            pltpu.VMEM((1, rows), F32),
            pltpu.VMEM((4 * cells, CHUNK), BF16),
            pltpu.VMEM((4 * cells, CHUNK), BF16),
            pltpu.VMEM((4 * cells, CHUNK), F8),
            pltpu.VMEM((4 * cells, CHUNK), F8),
            pltpu.VMEM((rows // CHUNK, nz, CHUNK), BF16),
            pltpu.VMEM((rows // CHUNK, nz, CHUNK), F8),
            pltpu.VMEM((4 * (cap // 128) * 16, 128), F32),
            pltpu.VMEM(density.shape, F32),
            pltpu.VMEM(density.shape, F32),
            pltpu.VMEM((4, 8, cap), F32),
            pltpu.VMEM((4, 8, cap), F32),
            pltpu.VMEM((4, cx, nz), F32),
            pltpu.VMEM((4, cx, nz), F32),
            pltpu.SemaphoreType.DMA((4,)),
            pltpu.SemaphoreType.DMA((4,)),
            pltpu.SemaphoreType.DMA((4,)),
            pltpu.SemaphoreType.DMA((4,)),
            pltpu.SemaphoreType.DMA((len(rounds),)),
            pltpu.SemaphoreType.DMA((len(rounds),)),
            pltpu.SMEM((1,), jnp.int32),
            pltpu.VMEM((1, rows), F32),
            pltpu.VMEM(velocity.shape, F32),
            pltpu.VMEM((1, rows), F32),
            pltpu.VMEM(cell.shape, jnp.int32),
            pltpu.SemaphoreType.DMA((8,)),
        ] + [pltpu.VMEM((len(group) + 1, 1, 128), F32) for group in rounds],
        compiler_params=pltpu.CompilerParams(
            collective_id=0, has_side_effects=True, vmem_limit_bytes=64200000
        ),
        name="spray",
    )(count, density, momentum, energy, mass.reshape(1, rows), velocity, temp.reshape(1, rows), cell)
    final = pl.pallas_call(
        put_out,
        out_shape=tuple(pltpu.HBM(o.shape, o.dtype) for o in outs),
        in_specs=[vmem] * 6,
        out_specs=(pl.BlockSpec(memory_space=pltpu.HBM),) * 6,
        scratch_shapes=[pltpu.SemaphoreType.DMA((6,))],
        compiler_params=pltpu.CompilerParams(vmem_limit_bytes=8 * 1024 * 1024),
        name="put_out",
    )(*outs)
    return tuple(final[:5]) + (final[5][0, 0],)


def solution(mesh):
    in_specs = (
        P("gx", "gy", None),
        P(None, "gx", "gy", None),
        P("gx", "gy", None),
        P(("gx", "gy")),
        P(None, ("gx", "gy")),
        P(("gx", "gy")),
        P(None, ("gx", "gy")),
        P(("gx", "gy")),
    )
    out_specs = (
        P("gx", "gy", None),
        P(None, "gx", "gy", None),
        P("gx", "gy", None),
        P(None, ("gx", "gy")),
        P(None, ("gx", "gy")),
        P(),
    )
    return jax.shard_map(
        functools.partial(on_device, mesh.shape["gx"], mesh.shape["gy"]),
        mesh=mesh, in_specs=in_specs, out_specs=out_specs, check_vma=False,
    )
```

```python
import functools

import jax
import jax.numpy as jnp
from jax import lax
from jax.experimental import pallas as pl
from jax.experimental.pallas import tpu as pltpu
from jax.sharding import PartitionSpec as P

ADIABATIC_INDEX = 1.4
KICK = 0.25
COURANT = 0.4
SHRINK = 0.5
MESH = pl.DeviceIdType.MESH
CHUNK = 1024
F32 = jnp.float32
BF16 = jnp.bfloat16
F8 = jnp.float8_e4m3fn
LIFT = 512.0
EDGES_AT = 2


def dot_nt(a, b):
    return lax.dot_general(a, b, (((1,), (1,)), ((), ())), preferred_element_type=F32)


def two_terms(x):
    high = x.astype(BF16)
    low = (x - high.astype(F32)).astype(BF16)
    return high, low


def one_hot_rows(row, count, hot=1.0):
    lanes = row.shape[1]
    base = (
        jnp.broadcast_to(row, (16, lanes))
        - lax.broadcasted_iota(jnp.int32, (16, lanes), 0).astype(F32)
    ).astype(BF16)
    one, zero = jnp.full((16, lanes), hot, BF16), jnp.zeros((16, lanes), BF16)
    return jnp.concatenate(
        [jnp.where(base == 16.0 * k, one, zero) for k in range(count // 16)], axis=0
    )


def peers_of(n_gx, n_gy):
    both = [(a, b) for b in range(n_gy) for a in range(n_gx) if a or b]
    both = both[n_gx - 1 :] + both[: n_gx - 1]
    if n_gx * n_gy <= 64:
        return (both,)
    return ([p for p in both if p[1] == 0], [p for p in both if p[0] == 0])


def kernel(
    n_gx, n_gy, count_hbm, density_hbm, momentum_hbm, energy_hbm, mass_hbm, vel_hbm, temp_hbm, cell_hbm,
    rho_ref, imp_ref, en_ref, state_ref, moved_ref, step_ref,
    upper_ref, src_ref, pay_ref, col_ref, q_ref, r_ref, a0_ref, a1_ref, c0_ref, c1_ref, b_ref, d_ref, small_ref, inv_ref, sound_ref,
    out_bucket, in_bucket, out_face, in_face,
    bucket_send, bucket_recv, face_send, face_recv, max_send, max_recv,
    count_ref, mass_ref, vel_ref, temp_ref, cell_ref, load_sem, *slots_refs,
):
    sources = (count_hbm, mass_hbm, temp_hbm, vel_hbm, cell_hbm, energy_hbm, density_hbm, momentum_hbm)
    places = (count_ref, mass_ref, temp_ref, vel_ref, cell_ref, en_ref, rho_ref, imp_ref)
    loads = []
    for k in range(8):
        load = pltpu.make_async_copy(sources[k], places[k], load_sem.at[k])
        load.start()
        loads.append(load)
    gx, gy = lax.axis_index("gx"), lax.axis_index("gy")
    cx, cy, nz = rho_ref.shape
    rows = mass_ref.shape[1]
    cap = rows // 16
    per = cap // 128
    cells = cx * cy
    chunks = rows // CHUNK
    i0 = lax.broadcasted_iota(jnp.int32, (128, 256), 0)
    i1 = lax.broadcasted_iota(jnp.int32, (128, 256), 1)
    upper_ref[...] = jnp.where((i0 < i1) | (i1 >= 128), 1.0, 0.0).astype(BF16)
    in_bucket[...] = jnp.zeros_like(in_bucket)
    in_face[...] = jnp.zeros_like(in_face)

    def peer(a, b):
        return {"gx": lax.rem(gx + a, n_gx), "gy": lax.rem(gy + b, n_gy)}

    rounds = peers_of(n_gx, n_gy)
    greeted = [p for group in rounds for p in group]
    barrier = pltpu.get_barrier_semaphore()
    for p in greeted:
        pl.semaphore_signal(barrier, inc=1, device_id=peer(*p), device_id_type=MESH)

    for load in loads[:5]:
        load.wait()
    blocks = CHUNK // 128

    def prepare(c, carry):
        lanes = pl.ds(c * CHUNK, CHUNK)
        mass, temp = mass_ref[:, lanes], temp_ref[:, lanes]
        live = lax.broadcasted_iota(jnp.int32, (1, CHUNK), 1) + c * CHUNK < count_ref[0]
        evap = jnp.where(live, LIFT * (mass * jax.nn.sigmoid(2.0 * (temp - 2.0))), 0.0)
        vx, vy, vz = vel_ref[0:1, lanes], vel_ref[1:2, lanes], vel_ref[2:3, lanes]
        src_ref[0:1, lanes] = evap
        src_ref[1:2, lanes] = evap * vx
        src_ref[2:3, lanes] = evap * vy
        src_ref[3:4, lanes] = evap * vz
        src_ref[4:5, lanes] = evap * (temp + 0.5 * (vx * vx + vy * vy + vz * vz))
        pay_ref[0:1, lanes] = mass - (SHRINK / LIFT) * evap
        pay_ref[1:4, lanes] = vel_ref[:, lanes]
        pay_ref[4:5, lanes] = temp
        pay_ref[5:8, lanes] = cell_ref[:, lanes].astype(F32)
        lx = cell_ref[0:1, lanes] - gx * cx
        ly = cell_ref[1:2, lanes] - gy * cy
        heading = jnp.where(
            lx < 0, 0, jnp.where(lx >= cx, 1, jnp.where(ly < 0, 2, jnp.where(ly >= cy, 3, 4)))
        )
        heading = jnp.where(live, heading, 5)
        col_ref[:, lanes] = jnp.where(heading == 4, lx * cy + ly, -1000).astype(F32)
        marks = jnp.where(
            jnp.broadcast_to(heading, (8, CHUNK)) == lax.broadcasted_iota(jnp.int32, (8, CHUNK), 0), 1.0, 0.0
        )
        stacked = jnp.concatenate([marks[:, k * 128 : (k + 1) * 128] for k in range(blocks)], axis=0)
        sums = jnp.dot(stacked.astype(BF16), upper_ref[...], preferred_element_type=F32)
        ranks = []
        for k in range(blocks):
            part = sums[k * 8 : (k + 1) * 8]
            mark = stacked[k * 8 : (k + 1) * 8]
            ranks.append(jnp.sum((part[:, :128] + carry) * mark, axis=0, keepdims=True))
            carry = carry + part[:, 128:]
        rank = jnp.concatenate(ranks, axis=1).astype(jnp.int32)
        q_ref[:, lanes] = jnp.where(heading < 4, heading * per + (rank >> 7), -1).astype(F32)
        r_ref[:, lanes] = (rank & 127).astype(F32)
        return carry

    groups = 4 * per
    small_ref[...] = jnp.zeros_like(small_ref)

    def columns(lanes):
        base = (
            jnp.broadcast_to(col_ref[:, lanes], (16, CHUNK))
            - lax.broadcasted_iota(jnp.int32, (16, CHUNK), 0).astype(F32)
        ).astype(BF16)
        return [base == 16.0 * k for k in range(cells // 16)]

    def spread(v, lanes, hits):
        zero = jnp.zeros((16, CHUNK), BF16)
        value = jnp.broadcast_to(src_ref[v : v + 1, lanes], (16, CHUNK))
        high = value.astype(BF16)
        low = (value - high.astype(F32)).astype(BF16)
        first = [jnp.where(hits[k], high, zero) for k in range(cells // 16)]
        second = [
            jnp.concatenate([jnp.where(hits[k], low, zero), jnp.where(hits[k + 1], low, zero)], axis=0).astype(F8)
            for k in range(0, cells // 16, 2)
        ]
        return first, second

    def front(c):
        lanes = pl.ds(c * CHUNK, CHUNK)
        high, low = two_terms(pay_ref[:, lanes])
        both = jnp.concatenate([high.astype(F32), low.astype(F32)], axis=0).astype(BF16)
        q = jnp.broadcast_to(q_ref[:, lanes], (16, CHUNK)).astype(BF16)
        zero = jnp.zeros((16, CHUNK), BF16)
        left = jnp.concatenate([jnp.where(q == float(k), both, zero) for k in range(groups)], axis=0)
        small_ref[...] += dot_nt(left, one_hot_rows(r_ref[:, lanes], 128))
        depth = one_hot_rows(cell_ref[2:3, lanes].astype(F32), nz, 1.0 / LIFT)
        unit = depth.astype(F8)
        b_ref[c] = depth
        d_ref[c] = unit
        first, second = spread(4, lanes, columns(lanes))
        part = dot_nt(jnp.concatenate(first, axis=0), depth) + dot_nt(jnp.concatenate(second, axis=0), unit)
        en_ref[...] += part.reshape(cx, cy, nz)

    count = jnp.zeros((8, 128), F32)
    count = prepare(0, count)
    count = prepare(1, count)
    loads[5].wait()
    for c in range(chunks):
        if c + 2 < chunks:
            count = prepare(c + 2, count)
        front(c)
    for h in range(4):
        for j in range(per):
            k = (h * per + j) * 16
            out_bucket[h, :, j * 128 : (j + 1) * 128] = small_ref[k : k + 8, :] + small_ref[k + 8 : k + 16, :]

    def build(c, a_ref, c_ref):
        lanes = pl.ds(c * CHUNK if isinstance(c, int) else pl.multiple_of(c * CHUNK, CHUNK), CHUNK)
        hits = columns(lanes)
        for v in range(4):
            first, second = spread(v, lanes, hits)
            for k in range(cells // 16):
                at = v * cells + k * 16
                a_ref[at : at + 16, :] = first[k]
            for k in range(cells // 32):
                at = v * cells + k * 32
                c_ref[at : at + 32, :] = second[k]

    build(0, a0_ref, c0_ref)

    pl.semaphore_wait(barrier, len(greeted))

    targets = (
        {"gx": lax.rem(gx + n_gx - 1, n_gx)},
        {"gx": lax.rem(gx + 1, n_gx)},
        {"gy": lax.rem(gy + n_gy - 1, n_gy)},
        {"gy": lax.rem(gy + 1, n_gy)},
    )
    there = (gx > 0, gx < n_gx - 1, gy > 0, gy < n_gy - 1)
    landing = (1, 0, 3, 2)

    def link(h, src, dst, send, recv):
        return pltpu.make_async_remote_copy(
            src_ref=src.at[h], dst_ref=dst.at[landing[h]], send_sem=send.at[h],
            recv_sem=recv.at[landing[h]], device_id=targets[h], device_id_type=MESH,
        )

    def launch(*refs):
        for h in range(4):
            pl.when(there[h])(lambda h=h: link(h, *refs).start())

    def arrive(*refs):
        for h in range(4):
            pl.when(there[landing[h]])(lambda h=h: link(h, *refs).wait_recv())

    def depart(*refs):
        for h in range(4):
            pl.when(there[h])(lambda h=h: link(h, *refs).wait_send())

    moves = (out_bucket, in_bucket, bucket_send, bucket_recv)
    faces = (out_face, in_face, face_send, face_recv)
    launch(*moves)
    for load in loads[6:]:
        load.wait()

    def edges():
        arrive(*moves)
        for b in range(4):
            got = in_bucket[b]
            warm = got[4:5]
            share = jax.nn.sigmoid(2.0 * (warm - 2.0))
            boiled = got[0:1] * share / (1.0 - SHRINK * share)
            speed = got[1:4]
            budget = 0.5 * jnp.sum(speed * speed, axis=0, keepdims=True)
            values = [boiled] + [boiled * got[k : k + 1] for k in (1, 2, 3)] + [boiled * (warm + budget)]
            if b < 2:
                along = got[6:7] - (gy * cy).astype(F32)
            else:
                along = got[5:6] - (gx * cx).astype(F32)
            hit = (
                jnp.broadcast_to(along, (16, cap))
                == lax.broadcasted_iota(jnp.int32, (16, cap), 0).astype(F32)
            )
            parts = []
            for value in values:
                wide = jnp.where(hit, jnp.broadcast_to(value, (16, cap)), 0.0)
                parts.append(two_terms(wide))
            left = jnp.concatenate([p[0] for p in parts] + [p[1] for p in parts], axis=0)
            sums = dot_nt(left, one_hot_rows(got[7:8], nz))
            sums = sums[0 : 5 * 16] + sums[5 * 16 : 10 * 16]
            fields = (rho_ref, imp_ref.at[0], imp_ref.at[1], imp_ref.at[2], en_ref)
            for v in range(5):
                part = sums[v * 16 : (v + 1) * 16]
                if b < 2:
                    x = 0 if b == 0 else cx - 1
                    fields[v][x] += part
                else:
                    y = 0 if b == 2 else cy - 1
                    for x in range(cx):
                        fields[v][x, y : y + 1, :] += part[x : x + 1]
        scale = ADIABATIC_INDEX - 1.0
        out_face[0] = scale * en_ref[0]
        out_face[1] = scale * en_ref[cx - 1]
        for x in range(cx):
            out_face[2, x : x + 1, :] = scale * en_ref[x, 0:1, :]
            out_face[3, x : x + 1, :] = scale * en_ref[x, cy - 1 : cy, :]
        launch(*faces)

    def add(c, a_ref, c_ref):
        part = dot_nt(a_ref[...], b_ref[c]) + dot_nt(c_ref[...], d_ref[c])
        rho_ref[...] += part[:cells].reshape(cx, cy, nz)
        imp_ref[...] += part[cells:].reshape(3, cx, cy, nz)

    half = 0.5 * KICK

    def kick():
        pressure = (ADIABATIC_INDEX - 1.0) * en_ref[...]
        lane = lax.broadcasted_iota(jnp.int32, (cx, cy, nz), 2)
        after = jnp.where(lane == nz - 1, 0.0, pltpu.roll(pressure, nz - 1, 2))
        before = jnp.where(lane == 0, 0.0, pltpu.roll(pressure, 1, 2))

        imp_ref[2] -= half * (after - before)
        line = lax.broadcasted_iota(jnp.int32, (cx, cy, nz), 1)
        after = jnp.where(line == cy - 1, 0.0, pltpu.roll(pressure, cy - 1, 1))
        before = jnp.where(line == 0, 0.0, pltpu.roll(pressure, 1, 1))
        imp_ref[1] -= half * (after - before)
        none = jnp.zeros((1, cy, nz), F32)
        after = jnp.concatenate([pressure[1:], none], axis=0)
        before = jnp.concatenate([none, pressure[:-1]], axis=0)
        imp_ref[0] -= half * (after - before)

    def two_chunks(i, carry):
        add(2 * i, a0_ref, c0_ref)
        build(2 * i + 1, a1_ref, c1_ref)
        add(2 * i + 1, a1_ref, c1_ref)
        build(2 * i + 2, a0_ref, c0_ref)
        return carry

    head = EDGES_AT
    lax.fori_loop(0, head, two_chunks, 0)
    edges()
    for c in range(2 * head, chunks):
        a_ref, c_ref = ((a0_ref, c0_ref), (a1_ref, c1_ref))[c % 2]
        add(c, a_ref, c_ref)
        if c + 1 < chunks:
            build(c + 1, *((a1_ref, c1_ref), (a0_ref, c0_ref))[c % 2])
        if c == 2 * head:
            kick()

    inverse = 1.0 / rho_ref[...]
    inv_ref[...] = inverse
    sound_ref[...] = jnp.sqrt(ADIABATIC_INDEX * (ADIABATIC_INDEX - 1.0) * en_ref[...] * inverse)
    arrive(*faces)
    imp_ref[0, 0] += half * in_face[0]
    imp_ref[0, cx - 1] -= half * in_face[1]
    for x in range(cx):
        imp_ref[1, x, 0:1, :] += half * in_face[2, x : x + 1, :]
        imp_ref[1, x, cy - 1 : cy, :] -= half * in_face[3, x : x + 1, :]
    fastest = jnp.maximum(jnp.maximum(jnp.abs(imp_ref[0]), jnp.abs(imp_ref[1])), jnp.abs(imp_ref[2]))
    wave = fastest * inv_ref[...] + sound_ref[...]
    wave = jnp.max(wave.reshape(cells, nz), axis=0, keepdims=True)
    top = functools.reduce(jnp.maximum, [wave[:, k * 128 : (k + 1) * 128] for k in range(nz // 128)])

    def settle():
        depart(*moves)
        depart(*faces)
        stays = col_ref[...] >= 0.0
        state_ref[:, :rows] = jnp.where(stays, pay_ref[0:5, :], 0.0)
        moved_ref[:, :rows] = jnp.where(stays, cell_ref[...], 0)
        for b in range(4):
            got = in_bucket[b]
            state_ref[:, rows + b * cap : rows + (b + 1) * cap] = got[0:5]
            moved_ref[:, rows + b * cap : rows + (b + 1) * cap] = got[5:8].astype(jnp.int32)

    def everyone(slots, sem):
        rest = slots.at[pl.ds(1, slots.shape[0] - 1)]
        return pltpu.make_async_copy(rest, rest, sem)

    for t, group in enumerate(rounds):
        slots = slots_refs[t]
        slots[0] = top
        for k, p in enumerate(group):
            pltpu.make_async_remote_copy(
                src_ref=slots.at[0], dst_ref=slots.at[k + 1], send_sem=max_send.at[t],
                recv_sem=max_recv.at[t], device_id=peer(*p), device_id_type=MESH,
            ).start()
        if t == 0:
            settle()
        everyone(slots, max_recv.at[t]).wait()
        top = jnp.max(slots[...], axis=0)
    step_ref[...] = COURANT / jnp.broadcast_to(jnp.max(top, axis=1, keepdims=True), (1, 128))
    for t in range(len(rounds)):
        everyone(slots_refs[t], max_send.at[t]).wait()


def put_out(*refs):
    count = (len(refs) - 1) // 2
    copies = []
    for k in range(count):
        copy = pltpu.make_async_copy(refs[k], refs[count + k], refs[-1].at[k])
        copy.start()
        copies.append(copy)
    for copy in copies:
        copy.wait()


def on_device(n_gx, n_gy, density, momentum, energy, mass, velocity, temp, cell, count):
    rows = mass.shape[0]
    cap = rows // 16
    slots = rows + 4 * cap
    cx, cy, nz = density.shape
    vmem = pl.BlockSpec(memory_space=pltpu.VMEM)
    cells = cx * cy
    rounds = peers_of(n_gx, n_gy)
    outs = pl.pallas_call(
        functools.partial(kernel, n_gx, n_gy),
        out_shape=(
            pltpu.VMEM(density.shape, F32),
            pltpu.VMEM(momentum.shape, F32),
            pltpu.VMEM(energy.shape, F32),
            pltpu.VMEM((5, slots), F32),
            pltpu.VMEM((3, slots), jnp.int32),
            pltpu.VMEM((1, 128), F32),
        ),
        in_specs=[pl.BlockSpec(memory_space=pltpu.HBM)] * 8,
        out_specs=(vmem,) * 6,
        scratch_shapes=[
            pltpu.VMEM((128, 256), BF16),
            pltpu.VMEM((8, rows), F32),
            pltpu.VMEM((8, rows), F32),
            pltpu.VMEM((1, rows), F32),
            pltpu.VMEM((1, rows), F32),
            pltpu.VMEM((1, rows), F32),
            pltpu.VMEM((4 * cells, CHUNK), BF16),
            pltpu.VMEM((4 * cells, CHUNK), BF16),
            pltpu.VMEM((4 * cells, CHUNK), F8),
            pltpu.VMEM((4 * cells, CHUNK), F8),
            pltpu.VMEM((rows // CHUNK, nz, CHUNK), BF16),
            pltpu.VMEM((rows // CHUNK, nz, CHUNK), F8),
            pltpu.VMEM((4 * (cap // 128) * 16, 128), F32),
            pltpu.VMEM(density.shape, F32),
            pltpu.VMEM(density.shape, F32),
            pltpu.VMEM((4, 8, cap), F32),
            pltpu.VMEM((4, 8, cap), F32),
            pltpu.VMEM((4, cx, nz), F32),
            pltpu.VMEM((4, cx, nz), F32),
            pltpu.SemaphoreType.DMA((4,)),
            pltpu.SemaphoreType.DMA((4,)),
            pltpu.SemaphoreType.DMA((4,)),
            pltpu.SemaphoreType.DMA((4,)),
            pltpu.SemaphoreType.DMA((len(rounds),)),
            pltpu.SemaphoreType.DMA((len(rounds),)),
            pltpu.SMEM((1,), jnp.int32),
            pltpu.VMEM((1, rows), F32),
            pltpu.VMEM(velocity.shape, F32),
            pltpu.VMEM((1, rows), F32),
            pltpu.VMEM(cell.shape, jnp.int32),
            pltpu.SemaphoreType.DMA((8,)),
        ] + [pltpu.VMEM((len(group) + 1, 1, 128), F32) for group in rounds],
        compiler_params=pltpu.CompilerParams(
            collective_id=0, has_side_effects=True, vmem_limit_bytes=64200000
        ),
        name="spray",
    )(count, density, momentum, energy, mass.reshape(1, rows), velocity, temp.reshape(1, rows), cell)
    final = pl.pallas_call(
        put_out,
        out_shape=tuple(pltpu.HBM(o.shape, o.dtype) for o in outs),
        in_specs=[vmem] * 6,
        out_specs=(pl.BlockSpec(memory_space=pltpu.HBM),) * 6,
        scratch_shapes=[pltpu.SemaphoreType.DMA((6,))],
        compiler_params=pltpu.CompilerParams(vmem_limit_bytes=8 * 1024 * 1024),
        name="put_out",
    )(*outs)
    return tuple(final[:5]) + (final[5][0, 0],)


def solution(mesh):
    in_specs = (
        P("gx", "gy", None),
        P(None, "gx", "gy", None),
        P("gx", "gy", None),
        P(("gx", "gy")),
        P(None, ("gx", "gy")),
        P(("gx", "gy")),
        P(None, ("gx", "gy")),
        P(("gx", "gy")),
    )
    out_specs = (
        P("gx", "gy", None),
        P(None, "gx", "gy", None),
        P("gx", "gy", None),
        P(None, ("gx", "gy")),
        P(None, ("gx", "gy")),
        P(),
    )
    return jax.shard_map(
        functools.partial(on_device, mesh.shape["gx"], mesh.shape["gy"]),
        mesh=mesh, in_specs=in_specs, out_specs=out_specs, check_vma=False,
    )
```
